32 devices in a mesh: batch: 8 (over y, x, core), seq: 4 (over z).
Axes of the slice: x: 2, y: 2, z: 4, core: 2. Of those that a mesh axis runs over, the one named last changes fastest.
Arguments:
- tokens: bfloat16 [8, 1024, 1024], P('batch', 'seq'), may hold values from -6 to 6
- doc_starts: int32 [8, 8], P('batch'), may hold values from 0 to 1023, as said below
- attention_gain: bfloat16 [1024], P(('batch', 'seq')), may hold values from 0.5 to 1.5
- attention_shift: bfloat16 [1024], P(('batch', 'seq')), may hold values from -3 to 3
- joint_weight: bfloat16 [1024, 3072], P(('batch', 'seq')), may hold values from -0.25 to 0.25
- joint_bias: bfloat16 [3072], P(('batch', 'seq')), may hold values from -3 to 3
- output_weight: bfloat16 [1024, 1024], P(('batch', 'seq')), may hold values from -0.5 to 0.5
- output_bias: bfloat16 [1024], P(('batch', 'seq')), may hold values from -3 to 3
- feed_gain: bfloat16 [1024], P(('batch', 'seq')), may hold values from 0.5 to 1.5
- feed_shift: bfloat16 [1024], P(('batch', 'seq')), may hold values from -3 to 3
- up_weight: bfloat16 [1024, 4096], P(('batch', 'seq')), may hold values from -0.1875 to 0.1875
- up_bias: bfloat16 [4096], P(('batch', 'seq')), may hold values from -3 to 3
- down_weight: bfloat16 [4096, 1024], P(('batch', 'seq')), may hold values from -0.125 to 0.125
- down_bias: bfloat16 [1024], P(('batch', 'seq')), may hold values from -3 to 3
- cotangent: bfloat16 [8, 1024, 1024], P('batch', 'seq'), may hold values from -6 to 6
Outputs:
- layer_out: bfloat16 [8, 1024, 1024], P('batch', 'seq')
- input_grad: float32 [8, 1024, 1024], P('batch', 'seq')
- attention_gain_grad: float32 [1024], P(('batch', 'seq'))
- attention_shift_grad: float32 [1024], P(('batch', 'seq'))
- joint_weight_grad: float32 [1024, 3072], P(('batch', 'seq'))
- joint_bias_grad: float32 [3072], P(('batch', 'seq'))
- output_weight_grad: float32 [1024, 1024], P(('batch', 'seq'))
- output_bias_grad: float32 [1024], P(('batch', 'seq'))
- feed_gain_grad: float32 [1024], P(('batch', 'seq'))
- feed_shift_grad: float32 [1024], P(('batch', 'seq'))
- up_weight_grad: float32 [1024, 4096], P(('batch', 'seq'))
- up_bias_grad: float32 [4096], P(('batch', 'seq'))
- down_weight_grad: float32 [4096, 1024], P(('batch', 'seq'))
- down_bias_grad: float32 [1024], P(('batch', 'seq'))
The draws below stay inside these ranges and needn't reach their ends.
Inputs may be any that keep to these rules, and one draw needn't show every extreme that they name: doc_starts[s, 0] is 0, each row does not fall, and its last entry is 1023; a document is the positions from one start to the next.
All inputs are finite; a program needn't handle non-finite values.
Results may differ from the reference program's by a relative error of at most 0.012.
Values may be sent and summed in bfloat16 or wider, within the bound.
A program may use at most 192 MiB of HBM per device.

```python
import jax
import jax.numpy as jnp
from jax import lax

D = 1024
HEADS = 16
HEAD_DIM = 64
ROT = 16
FF = 4096
DOCS = 8
STREAMS_ALL = 8
LEN = 1024


def draw_doc_starts(key, part):
    inner = jax.random.randint(key, (STREAMS_ALL, DOCS - 2), 1, LEN).astype(jnp.int32)
    last = jnp.full((STREAMS_ALL, 1), LEN - 1, jnp.int32)
    inner = jnp.sort(jnp.concatenate([inner, last], axis=1), axis=1)
    first = jnp.zeros((STREAMS_ALL, 1), jnp.int32)
    return jnp.concatenate([first, inner], axis=1).astype(jnp.int32)


def level_of(stream_key, extent, pieces, smallest, high):
    loudness, own = 1.0, jax.random.fold_in(stream_key, 6)
    for position, shards_of in pieces:
        steps = jnp.exp(jax.random.uniform(jax.random.fold_in(own, position), (shards_of,), jnp.float32, smallest / len(pieces), high / len(pieces)))
        loudness = loudness * jnp.repeat(steps, extent[position] // shards_of).reshape([-1 if axis == position else 1 for axis in range(len(extent))])
    return loudness


def gaussian(rng, extent, width, reach, split=(), kind=jnp.bfloat16):
    loudness = level_of(rng, extent, split, -0.22, 0.18) if split else 1.0
    values = jax.random.normal(rng, extent, jnp.float32) * width * loudness
    return jnp.minimum(jnp.maximum(values, -reach), reach).astype(kind)


def setup_inputs(seed: int = 0) -> dict:
    key_of = jax.random.split(jax.random.key(seed), 16)
    return {
        "tokens": gaussian(key_of[0], (STREAMS_ALL, LEN, D), 1.0, 6.0, ((0, 8), (1, 4))),
        "doc_starts": draw_doc_starts(jax.random.fold_in(key_of[15], 71), 0),
        "attention_gain": jnp.clip(1.0 + 0.1 * jax.random.normal(key_of[2], (D,), jnp.float32), 0.5, 1.5).astype(jnp.bfloat16),
        "attention_shift": gaussian(key_of[3], (D,), 0.2, 3.0, ((0, 32),)),
        "joint_weight": gaussian(key_of[4], (D, 3 * D), (D // 2) ** -0.5, 0.25, ((0, 32),)),
        "joint_bias": gaussian(key_of[5], (3 * D,), 0.2, 3.0, ((0, 32),)),
        "output_weight": gaussian(key_of[6], (D, D), (D // 8) ** -0.5, 0.5, ((0, 32),)),
        "output_bias": gaussian(key_of[7], (D,), 0.2, 3.0, ((0, 32),)),
        "feed_gain": jnp.clip(1.0 + 0.1 * jax.random.normal(key_of[8], (D,), jnp.float32), 0.5, 1.5).astype(jnp.bfloat16),
        "feed_shift": gaussian(key_of[9], (D,), 0.2, 3.0, ((0, 32),)),
        "up_weight": gaussian(key_of[10], (D, FF), D ** -0.5, 0.1875, ((0, 32),)),
        "up_bias": gaussian(key_of[11], (FF,), 0.2, 3.0, ((0, 32),)),
        "down_weight": gaussian(key_of[12], (FF, D), (FF // 2) ** -0.5, 0.125, ((0, 32),)),
        "down_bias": gaussian(key_of[13], (D,), 0.2, 3.0, ((0, 32),)),
        "cotangent": gaussian(key_of[14], (STREAMS_ALL, LEN, D), 1.0, 6.0, ((0, 8), (1, 4))),
    }


@jax.custom_vjp
def low(v):
    return lax.optimization_barrier(v.astype(jnp.bfloat16)).astype(jnp.float32)

@jax.custom_vjp
def low_back(v):
    return v

def low_keep(v):
    return (low(v), None)

def low_pass(kept, grad):
    return (grad,)

def back_keep(v):
    return (v, None)

def back_low(kept, grad):
    return (low(grad),)
low.defvjp(low_keep, low_pass)
low_back.defvjp(back_keep, back_low)
highest = lax.Precision.HIGHEST
block_rows = 512

def norm_rows(values, gain, shift):
    centred = values - lax.optimization_barrier(jnp.mean(values, axis=-1, keepdims=True))
    spread = lax.optimization_barrier(jnp.mean(centred * centred, axis=-1, keepdims=True))
    return centred * lax.rsqrt(spread + 1e-05) * gain + shift

def angle_tables(places):
    half = ROT // 2
    inverse = 10000.0 ** (-(jnp.arange(half, dtype=jnp.float32) * 2.0) / ROT)
    angles = places.astype(jnp.float32)[:, None] * inverse[None, :]
    return (jnp.cos(angles)[:, None, :], jnp.sin(angles)[:, None, :])

def rotate(vectors, cosine, sine, sign):
    half = ROT // 2
    front = vectors[..., :half]
    behind = vectors[..., half:ROT]
    new_front = front * cosine - sign * behind * sine
    new_behind = behind * cosine + sign * front * sine
    return jnp.concatenate([new_front, new_behind, vectors[..., ROT:]], axis=-1)

def segment_ids(starts, length):
    places = jnp.arange(length, dtype=jnp.int32)
    return lax.optimization_barrier(jnp.sum((starts[None, :] <= places[:, None]).astype(jnp.int32), axis=1))

def attend(query, keys, values, segment):
    rows = min(block_rows, LEN)
    places = jnp.arange(LEN, dtype=jnp.int32)
    scale = HEAD_DIM ** (-0.5)

    def one_block(index):
        start = (index * rows).astype(jnp.int32)
        picked = lax.dynamic_slice_in_dim(query, start, rows, 0)
        query_places = lax.dynamic_slice_in_dim(places, start, rows, 0)
        query_segment = lax.dynamic_slice_in_dim(segment, start, rows, 0)
        allowed = (places[None, :] <= query_places[:, None]) & (segment[None, :] == query_segment[:, None])
        scores = low_back(jnp.einsum('qhd,khd->hqk', picked, keys, precision=highest) * scale)
        probs = jax.nn.softmax(jnp.where(allowed[None], scores, -1e+30), axis=-1)
        return jnp.einsum('hqk,khd->qhd', low(probs), values, precision=highest)
    blocks = lax.map(jax.checkpoint(one_block), jnp.arange(LEN // rows, dtype=jnp.int32))
    return blocks.reshape(LEN, query.shape[1], HEAD_DIM)

def one_stream(tokens, starts, weights):
    attention_gain, attention_shift, joint_weight, joint_bias, output_weight, output_bias, feed_gain, feed_shift, up_weight, up_bias, down_weight, down_bias = weights
    first = low(norm_rows(tokens, attention_gain, attention_shift))
    second = low(norm_rows(tokens, feed_gain, feed_shift))
    mixed = low_back(jnp.dot(first, joint_weight, precision=highest) + joint_bias)
    mixed = mixed.reshape(LEN, 3, HEADS, HEAD_DIM)
    cosine, sine = angle_tables(jnp.arange(LEN, dtype=jnp.int32))
    query = low_back(low(rotate(mixed[:, 0], cosine, sine, 1.0)))
    keys = low_back(low(rotate(mixed[:, 1], cosine, sine, 1.0)))
    values = low_back(low(mixed[:, 2]))
    heads = attend(query, keys, values, segment_ids(starts, LEN))
    merged = low_back(low(heads.reshape(LEN, D)))
    attention = jnp.dot(merged, output_weight, precision=highest) + output_bias
    up = low_back(jnp.dot(second, up_weight, precision=highest) + up_bias)
    active = low(jax.nn.gelu(up, approximate=False))
    feed = jnp.dot(active, down_weight, precision=highest) + down_bias
    return tokens + attention + feed

def reference(tokens, doc_starts, attention_gain, attention_shift, joint_weight, joint_bias, output_weight, output_bias, feed_gain, feed_shift, up_weight, up_bias, down_weight, down_bias, cotangent):
    weights = tuple((item.astype(jnp.float32) for item in (attention_gain, attention_shift, joint_weight, joint_bias, output_weight, output_bias, feed_gain, feed_shift, up_weight, up_bias, down_weight, down_bias)))
    stream_step = jax.checkpoint(one_stream)

    def forward(inputs, params):
        return lax.map(lambda pair: stream_step(pair[0], pair[1], params), (inputs, doc_starts))
    layer_out, pullback = jax.vjp(forward, tokens.astype(jnp.float32), weights)
    input_grad, grads = pullback(cotangent.astype(jnp.float32))
    return (layer_out.astype(jnp.bfloat16), input_grad, grads[0], grads[1], grads[2], grads[3], grads[4], grads[5], grads[6], grads[7], grads[8], grads[9], grads[10], grads[11])
```

```python
import jax
import jax.numpy as jnp
from jax import lax
from jax.sharding import PartitionSpec as P

HEADS = 16
HEAD_DIM = 64
ROT = 16
BLOCK_ROWS = 512
F32 = jnp.float32
BF16 = jnp.bfloat16


def dot(a, b, dims):
    return lax.dot_general(a, b, (dims, ((), ())), preferred_element_type=F32)


def normalised(values):
    centred = values - jnp.mean(values, axis=-1, keepdims=True)
    spread = jnp.mean(centred * centred, axis=-1, keepdims=True)
    scale = lax.rsqrt(spread + 1e-05)
    return centred * scale, scale


def angle_tables(places):
    half = ROT // 2
    inverse = 10000.0 ** (-(jnp.arange(half, dtype=F32) * 2.0) / ROT)
    angles = places.astype(F32)[:, None] * inverse[None, :]
    return (jnp.cos(angles)[:, None, :], jnp.sin(angles)[:, None, :])


def rotate(vectors, cosine, sine, sign):
    half = ROT // 2
    front = vectors[..., :half]
    behind = vectors[..., half:ROT]
    new_front = front * cosine - sign * behind * sine
    new_behind = behind * cosine + sign * front * sine
    return jnp.concatenate([new_front, new_behind, vectors[..., ROT:]], axis=-1)


def allowed_block(places, segment, start, rows):
    query_places = lax.dynamic_slice_in_dim(places, start, rows, 0)
    query_segment = lax.dynamic_slice_in_dim(segment, start, rows, 0)
    return (places[None, :] <= query_places[:, None]) & (segment[None, :] == query_segment[:, None])


def forward_stream(query, keys, values, segment, scale):
    full_len = query.shape[0]
    rows = min(BLOCK_ROWS, full_len)
    places = jnp.arange(full_len, dtype=jnp.int32)

    def one_block(index):
        start = index * rows
        picked = lax.dynamic_slice_in_dim(query, start, rows, 0)
        allowed = allowed_block(places, segment, start, rows)
        scores = jnp.einsum("qhd,khd->hqk", picked, keys, preferred_element_type=F32) * scale
        masked = jnp.where(allowed[None], scores, -1e30)
        top = jnp.max(masked, axis=-1, keepdims=True)
        weights = jnp.exp(masked - top)
        total = jnp.sum(weights, axis=-1, keepdims=True)
        probs = (weights / total).astype(BF16)
        result = jnp.einsum("hqk,khd->qhd", probs, values, preferred_element_type=F32)
        return (result.astype(BF16), (top + jnp.log(total))[:, :, 0])

    results, sums_log = lax.map(one_block, jnp.arange(full_len // rows, dtype=jnp.int32))
    return (results.reshape(query.shape), sums_log)


def backward_stream(query, keys, values, segment, sums_log, grad_out, scale):
    full_len = query.shape[0]
    rows = min(BLOCK_ROWS, full_len)
    places = jnp.arange(full_len, dtype=jnp.int32)

    def one_block(carry, index):
        key_grad, value_grad = carry
        start = index * rows
        picked = lax.dynamic_slice_in_dim(query, start, rows, 0)
        grad_rows = lax.dynamic_slice_in_dim(grad_out, start, rows, 0)
        allowed = allowed_block(places, segment, start, rows)
        scores = jnp.einsum("qhd,khd->hqk", picked, keys, preferred_element_type=F32) * scale
        masked = jnp.where(allowed[None], scores, -1e30)
        probs = jnp.exp(masked - sums_log[index][:, :, None])
        value_grad = value_grad + jnp.einsum(
            "hqk,qhd->khd", probs.astype(BF16), grad_rows, preferred_element_type=F32
        )
        prob_grad = jnp.einsum("qhd,khd->hqk", grad_rows, values, preferred_element_type=F32)
        inner = jnp.sum(probs * prob_grad, axis=-1, keepdims=True)
        score_grad = (probs * (prob_grad - inner)).astype(BF16)
        query_grad = (
            jnp.einsum("hqk,khd->qhd", score_grad, keys, preferred_element_type=F32) * scale
        )
        key_grad = (
            key_grad
            + jnp.einsum("hqk,qhd->khd", score_grad, picked, preferred_element_type=F32) * scale
        )
        return ((key_grad, value_grad), query_grad.astype(BF16))

    empty = jnp.zeros(keys.shape, F32)
    (key_grad, value_grad), query_grads = lax.scan(
        one_block, (empty, empty), jnp.arange(full_len // rows, dtype=jnp.int32)
    )
    return (query_grads.reshape(query.shape), key_grad.astype(BF16), value_grad.astype(BF16))


def body(
    tokens,
    doc_starts,
    attention_gain,
    attention_shift,
    joint_weight,
    joint_bias,
    output_weight,
    output_bias,
    feed_gain,
    feed_shift,
    up_weight,
    up_bias,
    down_weight,
    down_bias,
    cotangent,
):
    streams, local_len, width = tokens.shape
    batch_size, seq_size = lax.axis_size("batch"), lax.axis_size("seq")
    devices = batch_size * seq_size
    seq_index = lax.axis_index("seq")
    full_len = local_len * seq_size
    count = streams * full_len
    local_heads = HEADS // seq_size
    head_width = local_heads * HEAD_DIM
    rows = joint_weight.shape[0]
    hidden_rows = down_weight.shape[0]
    hidden = hidden_rows * batch_size
    scale = HEAD_DIM ** (-0.5)
    both = ("batch", "seq")

    vectors = (
        attention_gain, attention_shift, output_bias, feed_gain, feed_shift, down_bias, joint_bias, up_bias,
    )
    packed = jnp.concatenate(vectors)
    sizes = [v.shape[0] for v in vectors]
    everyone = lax.all_gather(packed[None], both, axis=0, tiled=True)
    parts, at = [], 0
    for size in sizes:
        parts.append(everyone[:, at : at + size].astype(F32))
        at += size
    gain_a, shift_a, bias_o, gain_f, shift_f, bias_d, bias_j, bias_u = parts
    gain_a, shift_a, bias_o, gain_f, shift_f, bias_d, bias_j = (
        v.reshape(-1) for v in (gain_a, shift_a, bias_o, gain_f, shift_f, bias_d, bias_j)
    )
    bias_j = lax.dynamic_index_in_dim(
        bias_j.reshape(3, seq_size, head_width), seq_index, 1, keepdims=False
    ).reshape(-1)
    bias_u = lax.dynamic_index_in_dim(
        bias_u.reshape(batch_size, seq_size, hidden_rows), seq_index, 1, keepdims=False
    ).reshape(-1)

    def column_gather(weight, split):
        moved = lax.all_to_all(split, "seq", split_axis=0, concat_axis=0, tiled=True)
        return lax.all_gather(moved.reshape(seq_size * rows, -1), "batch", axis=0, tiled=True)

    full_tokens = lax.all_gather(tokens, "seq", axis=1, tiled=True).reshape(count, width)
    joint = column_gather(
        joint_weight,
        joint_weight.reshape(rows, 3, seq_size, head_width).transpose(2, 0, 1, 3).reshape(seq_size, rows, -1),
    )
    up_w = column_gather(
        up_weight,
        up_weight.reshape(rows, batch_size, seq_size, hidden_rows)
        .transpose(2, 0, 1, 3)
        .reshape(seq_size, rows, -1),
    )
    down_w = lax.all_gather(down_weight, "batch", axis=0, tiled=True)
    there = []
    for b in range(batch_size):
        for s in range(seq_size):
            r = b * seq_size + s
            there.append((r, (r % batch_size) * seq_size + r // batch_size))
    back = [(d, r) for r, d in there]
    out_w = lax.all_gather(
        lax.ppermute(output_weight, both, there), "batch", axis=0, tiled=True
    )
    grad = lax.all_gather(cotangent, "seq", axis=1, tiled=True).reshape(count, width)

    rows_f32 = full_tokens.astype(F32)
    unit, _ = normalised(rows_f32)
    first = (unit * gain_a + shift_a).astype(BF16)
    second = (unit * gain_f + shift_f).astype(BF16)
    mixed = dot(first, joint, ((1,), (0,))) + bias_j
    mixed = mixed.reshape(streams, full_len, 3, local_heads, HEAD_DIM)
    cosine, sine = angle_tables(jnp.arange(full_len, dtype=jnp.int32))
    query = rotate(mixed[:, :, 0], cosine, sine, 1.0).astype(BF16)
    keys = rotate(mixed[:, :, 1], cosine, sine, 1.0).astype(BF16)
    values = mixed[:, :, 2].astype(BF16)
    places = jnp.arange(full_len, dtype=jnp.int32)
    segment = jnp.sum((doc_starts[:, None, :] <= places[None, :, None]).astype(jnp.int32), axis=2)
    heads_out, sums_log = lax.map(
        lambda item: forward_stream(*item, scale), (query, keys, values, segment)
    )
    merged = heads_out.reshape(count, head_width)
    up = dot(second, up_w, ((1,), (0,))) + bias_u
    active_f32, gelu_pullback = jax.vjp(lambda v: jax.nn.gelu(v, approximate=False), up)
    active = active_f32.astype(BF16)
    partial_out = dot(merged, out_w, ((1,), (0,))) + dot(active, down_w, ((1,), (0,)))
    summed_out = lax.psum_scatter(
        partial_out.astype(BF16).reshape(streams, full_len, width), "seq", scatter_dimension=1, tiled=True
    )
    layer_out = (tokens.astype(F32) + summed_out.astype(F32) + (bias_o + bias_d)).astype(BF16)

    active_grad = dot(grad, down_w, ((1,), (1,)))
    up_grad = gelu_pullback(active_grad)[0].astype(BF16)
    second_grad = dot(up_grad, up_w, ((1,), (1,)))
    down_grad = dot(active, grad, ((0,), (0,)))
    up_weight_grad = dot(second, up_grad, ((0,), (0,)))
    output_weight_grad = dot(merged, grad, ((0,), (0,)))
    heads_grad = dot(grad, out_w, ((1,), (1,))).astype(BF16)
    heads_grad = heads_grad.reshape(streams, full_len, local_heads, HEAD_DIM)
    query_grad, key_grad, value_grad = lax.map(
        lambda item: backward_stream(*item, scale),
        (query, keys, values, segment, sums_log, heads_grad),
    )
    query_back = rotate(query_grad.astype(F32), cosine, sine, -1.0).astype(BF16)
    keys_back = rotate(key_grad.astype(F32), cosine, sine, -1.0).astype(BF16)
    mixed_grad = jnp.stack([query_back, keys_back, value_grad], axis=2).reshape(count, 3 * head_width)
    joint_weight_grad = dot(first, mixed_grad, ((0,), (0,)))
    first_grad = dot(mixed_grad, joint, ((1,), (1,)))

    incoming = first_grad * gain_a + second_grad * gain_f
    incoming = lax.psum_scatter(
        incoming.astype(BF16).reshape(streams, full_len, width), "seq", scatter_dimension=1, tiled=True
    ).astype(F32)
    own_unit, own_scale = normalised(tokens.astype(F32))
    own_term = own_scale * (
        incoming
        - jnp.mean(incoming, axis=-1, keepdims=True)
        - own_unit * jnp.mean(incoming * own_unit, axis=-1, keepdims=True)
    )
    input_grad = cotangent.astype(F32) + own_term

    def scatter_rows(value):
        return lax.psum_scatter(value.astype(BF16), "batch", scatter_dimension=0, tiled=True)

    def column_scatter(value):
        moved = scatter_rows(value).reshape(seq_size, rows, -1)
        return lax.all_to_all(moved, "seq", split_axis=0, concat_axis=0, tiled=True).astype(F32)

    joint_out = (
        column_scatter(joint_weight_grad)
        .reshape(seq_size, rows, 3, head_width)
        .transpose(1, 2, 0, 3)
        .reshape(rows, -1)
    )
    up_out = (
        column_scatter(up_weight_grad)
        .reshape(seq_size, rows, batch_size, hidden_rows)
        .transpose(1, 2, 0, 3)
        .reshape(rows, -1)
    )
    down_out = scatter_rows(down_grad).astype(F32)
    output_out = lax.ppermute(scatter_rows(output_weight_grad), both, back).astype(F32)

    own = (jnp.arange(seq_size) == seq_index).astype(F32)
    joint_bias_sum = jnp.sum(mixed_grad.astype(F32), axis=0).reshape(3, 1, head_width) * own[None, :, None]
    up_bias_sum = jnp.sum(up_grad.astype(F32), axis=0).reshape(batch_size, 1, hidden_rows) * own[None, :, None]
    sums = (
        jnp.sum(first_grad * unit, axis=0),
        jnp.sum(first_grad, axis=0),
        jnp.sum(cotangent.astype(F32), axis=(0, 1)),
        jnp.sum(second_grad * unit, axis=0),
        jnp.sum(second_grad, axis=0),
        joint_bias_sum.reshape(-1),
        up_bias_sum.reshape(-1),
    )
    grouped = jnp.concatenate([s.reshape(devices, -1) for s in sums], axis=1)
    mine = lax.psum_scatter(grouped, both, scatter_dimension=0, tiled=True)[0]
    small, at = [], 0
    for value in sums:
        size = value.shape[0] // devices
        small.append(mine[at : at + size])
        at += size
    return (
        layer_out,
        input_grad,
        small[0],
        small[1],
        joint_out,
        small[5],
        output_out,
        small[2],
        small[3],
        small[4],
        up_out,
        small[6],
        down_out,
        small[2],
    )


def solution(mesh):
    split = P(("batch", "seq"))
    matrix = P(("batch", "seq"), None)
    rows = P("batch", "seq", None)
    return jax.shard_map(
        body,
        mesh=mesh,
        in_specs=(
            rows, P("batch", None), split, split, matrix, split, matrix, split, split, split, matrix, split,
            matrix, split, rows,
        ),
        out_specs=(
            rows, rows, split, split, matrix, split, matrix, split, split, split, matrix, split, matrix, split,
        ),
        check_vma=False,
    )
```

```python
import jax
import jax.numpy as jnp
from jax import lax
from jax.sharding import PartitionSpec as P

HEADS = 16
HEAD_DIM = 64
ROT = 16
BLOCK_ROWS = 512
F32 = jnp.float32
BF16 = jnp.bfloat16


def dot(a, b, dims):
    return lax.dot_general(a, b, (dims, ((), ())), preferred_element_type=F32)


def normalised(values):
    centred = values - jnp.mean(values, axis=-1, keepdims=True)
    spread = jnp.mean(centred * centred, axis=-1, keepdims=True)
    scale = lax.rsqrt(spread + 1e-05)
    return centred * scale, scale


def angle_tables(places):
    half = ROT // 2
    inverse = 10000.0 ** (-(jnp.arange(half, dtype=F32) * 2.0) / ROT)
    angles = places.astype(F32)[:, None] * inverse[None, :]
    return (jnp.cos(angles)[:, None, :], jnp.sin(angles)[:, None, :])


def rotate(vectors, cosine, sine, sign):
    half = ROT // 2
    front = vectors[..., :half]
    behind = vectors[..., half:ROT]
    new_front = front * cosine - sign * behind * sine
    new_behind = behind * cosine + sign * front * sine
    return jnp.concatenate([new_front, new_behind, vectors[..., ROT:]], axis=-1)


def allowed_block(places, segment, start, rows):
    query_places = lax.dynamic_slice_in_dim(places, start, rows, 0)
    query_segment = lax.dynamic_slice_in_dim(segment, start, rows, 0)
    return (places[None, :] <= query_places[:, None]) & (segment[None, :] == query_segment[:, None])


def forward_stream(query, keys, values, segment, scale):
    full_len = query.shape[0]
    rows = min(BLOCK_ROWS, full_len)
    places = jnp.arange(full_len, dtype=jnp.int32)

    def one_block(index):
        start = index * rows
        picked = lax.dynamic_slice_in_dim(query, start, rows, 0)
        allowed = allowed_block(places, segment, start, rows)
        scores = jnp.einsum("qhd,khd->hqk", picked, keys, preferred_element_type=F32) * scale
        masked = jnp.where(allowed[None], scores, -1e30)
        top = jnp.max(masked, axis=-1, keepdims=True)
        weights = jnp.exp(masked - top)
        total = jnp.sum(weights, axis=-1, keepdims=True)
        probs = (weights / total).astype(BF16)
        result = jnp.einsum("hqk,khd->qhd", probs, values, preferred_element_type=F32)
        return (result.astype(BF16), (top + jnp.log(total))[:, :, 0])

    results, sums_log = lax.map(one_block, jnp.arange(full_len // rows, dtype=jnp.int32))
    return (results.reshape(query.shape), sums_log)


def backward_stream(query, keys, values, segment, sums_log, grad_out, scale):
    full_len = query.shape[0]
    rows = min(BLOCK_ROWS, full_len)
    places = jnp.arange(full_len, dtype=jnp.int32)

    def one_block(carry, index):
        key_grad, value_grad = carry
        start = index * rows
        picked = lax.dynamic_slice_in_dim(query, start, rows, 0)
        grad_rows = lax.dynamic_slice_in_dim(grad_out, start, rows, 0)
        allowed = allowed_block(places, segment, start, rows)
        scores = jnp.einsum("qhd,khd->hqk", picked, keys, preferred_element_type=F32) * scale
        masked = jnp.where(allowed[None], scores, -1e30)
        probs = jnp.exp(masked - sums_log[index][:, :, None])
        value_grad = value_grad + jnp.einsum(
            "hqk,qhd->khd", probs.astype(BF16), grad_rows, preferred_element_type=F32
        )
        prob_grad = jnp.einsum("qhd,khd->hqk", grad_rows, values, preferred_element_type=F32)
        inner = jnp.sum(probs * prob_grad, axis=-1, keepdims=True)
        score_grad = (probs * (prob_grad - inner)).astype(BF16)
        query_grad = (
            jnp.einsum("hqk,khd->qhd", score_grad, keys, preferred_element_type=F32) * scale
        )
        key_grad = (
            key_grad
            + jnp.einsum("hqk,qhd->khd", score_grad, picked, preferred_element_type=F32) * scale
        )
        return ((key_grad, value_grad), query_grad.astype(BF16))

    empty = jnp.zeros(keys.shape, F32)
    (key_grad, value_grad), query_grads = lax.scan(
        one_block, (empty, empty), jnp.arange(full_len // rows, dtype=jnp.int32)
    )
    return (query_grads.reshape(query.shape), key_grad.astype(BF16), value_grad.astype(BF16))


def bit_list(name):
    size, bits, bit = lax.axis_size(name), [], 1
    while bit < size:
        bits.append(bit)
        bit *= 2
    return bits


def swap(value, name, bit):
    return lax.ppermute(value, name, [(i, i ^ bit) for i in range(lax.axis_size(name))])


def high_half(name, bit):
    return (lax.axis_index(name) // bit) % 2 == 1


def gather_bits(value, name, order):
    shape, done, current = value.shape, [], value
    for bit in order:
        other = swap(current, name, bit)
        upper = high_half(name, bit)
        place = sum(1 for known in done if known > bit)
        done.append(bit)
        current = jnp.stack(
            [jnp.where(upper, other, current), jnp.where(upper, current, other)], axis=place
        )
    return current.reshape((lax.axis_size(name),) + shape)


def scatter_bits(value, name, order, wire):
    dims = sorted(order, reverse=True)
    current = value.reshape((2,) * len(dims) + value.shape[1:])
    for bit in order:
        place = dims.index(bit)
        dims.remove(bit)
        low = lax.index_in_dim(current, 0, place, keepdims=False)
        high = lax.index_in_dim(current, 1, place, keepdims=False)
        upper = high_half(name, bit)
        other = swap(jnp.where(upper, low, high).astype(wire), name, bit)
        current = jnp.where(upper, high, low) + other.astype(F32)
    return current


def exchange(value, name):
    size, index = lax.axis_size(name), lax.axis_index(name)
    pieces = [lax.dynamic_index_in_dim(value, index, 0, keepdims=False)]
    for step in range(1, size):
        block = lax.dynamic_index_in_dim(value, (index + step) % size, 0, keepdims=False)
        pieces.append(lax.ppermute(block, name, [(i, (i + step) % size) for i in range(size)]))
    turned = [pieces[0]] + pieces[:0:-1]
    return lax.dynamic_slice_in_dim(jnp.stack(turned + turned), (size - index) % size, size, 0)


def gather_line(block, name):
    size, index = lax.axis_size(name), lax.axis_index(name)
    up = [(i, i + 1) for i in range(size - 1)]
    down = [(i + 1, i) for i in range(size - 1)]
    below, above = [block], [block]
    for _ in range(size - 1):
        below.append(lax.ppermute(below[-1], name, up))
        above.append(lax.ppermute(above[-1], name, down))
    row = jnp.stack(below[:0:-1] + above)
    return lax.dynamic_slice_in_dim(row, size - 1 - index, size, 0)


def scatter_direct(value, name):
    size, index = lax.axis_size(name), lax.axis_index(name)
    total = lax.dynamic_index_in_dim(value, index, 0, keepdims=False).astype(F32)
    for step in range(1, size):
        block = lax.dynamic_index_in_dim(value, (index + step) % size, 0, keepdims=False)
        other = lax.ppermute(block.astype(BF16), name, [(i, (i + step) % size) for i in range(size)])
        total = total + other.astype(F32)
    return total


def body(
    tokens,
    doc_starts,
    attention_gain,
    attention_shift,
    joint_weight,
    joint_bias,
    output_weight,
    output_bias,
    feed_gain,
    feed_shift,
    up_weight,
    up_bias,
    down_weight,
    down_bias,
    cotangent,
):
    streams, local_len, width = tokens.shape
    batch_size, seq_size = lax.axis_size("batch"), lax.axis_size("seq")
    devices = batch_size * seq_size
    seq_index = lax.axis_index("seq")
    full_len = local_len * seq_size
    assert streams == 1
    count = streams * full_len
    local_heads = HEADS // seq_size
    head_width = local_heads * HEAD_DIM
    rows = joint_weight.shape[0]
    hidden_rows = down_weight.shape[0]
    hidden = hidden_rows * batch_size
    scale = HEAD_DIM ** (-0.5)
    both = ("batch", "seq")

    vectors = (
        attention_gain, attention_shift, output_bias, feed_gain, feed_shift, down_bias, joint_bias, up_bias,
    )
    packed = jnp.concatenate(vectors)
    sizes = [v.shape[0] for v in vectors]
    batch_bits, seq_bits = bit_list("batch"), bit_list("seq")
    first_route = batch_bits[1:] + batch_bits[:1]
    second_route = batch_bits[2:] + batch_bits[1:2] + batch_bits[:1]
    everyone = gather_bits(gather_bits(packed, "seq", seq_bits), "batch", first_route)
    everyone = everyone.reshape(devices, -1)
    parts, at = [], 0
    for size in sizes:
        parts.append(everyone[:, at : at + size].astype(F32))
        at += size
    gain_a, shift_a, bias_o, gain_f, shift_f, bias_d, bias_j, bias_u = parts
    gain_a, shift_a, bias_o, gain_f, shift_f, bias_d, bias_j = (
        v.reshape(-1) for v in (gain_a, shift_a, bias_o, gain_f, shift_f, bias_d, bias_j)
    )
    bias_j = lax.dynamic_index_in_dim(
        bias_j.reshape(3, seq_size, head_width), seq_index, 1, keepdims=False
    ).reshape(-1)
    bias_u = lax.dynamic_index_in_dim(
        bias_u.reshape(batch_size, seq_size, hidden_rows), seq_index, 1, keepdims=False
    ).reshape(-1)

    full_tokens = gather_line(tokens.reshape(-1, width), "seq").reshape(count, width)
    joint_rows = exchange(
        joint_weight.reshape(rows, 3, seq_size, head_width).transpose(2, 0, 1, 3).reshape(seq_size, rows, -1),
        "seq",
    )
    joint = gather_bits(joint_rows, "batch", first_route).reshape(width, -1)
    up_rows = exchange(
        up_weight.reshape(rows, batch_size, seq_size, hidden_rows)
        .transpose(2, 0, 1, 3)
        .reshape(seq_size, rows, -1),
        "seq",
    )
    up_w = gather_bits(up_rows, "batch", second_route).reshape(width, -1)
    down_w = gather_bits(down_weight, "batch", second_route).reshape(hidden, width)
    there = []
    for b in range(batch_size):
        for s in range(seq_size):
            r = b * seq_size + s
            there.append((r, (r % batch_size) * seq_size + r // batch_size))
    back = [(d, r) for r, d in there]
    out_w = gather_bits(lax.ppermute(output_weight, both, there), "batch", first_route).reshape(head_width, width)
    grad = gather_line(cotangent.reshape(-1, width), "seq").reshape(count, width)

    rows_f32 = full_tokens.astype(F32)
    unit, _ = normalised(rows_f32)
    first = (unit * gain_a + shift_a).astype(BF16)
    second = (unit * gain_f + shift_f).astype(BF16)
    mixed = dot(first, joint, ((1,), (0,))) + bias_j
    mixed = mixed.reshape(streams, full_len, 3, local_heads, HEAD_DIM)
    cosine, sine = angle_tables(jnp.arange(full_len, dtype=jnp.int32))
    query = rotate(mixed[:, :, 0], cosine, sine, 1.0).astype(BF16)
    keys = rotate(mixed[:, :, 1], cosine, sine, 1.0).astype(BF16)
    values = mixed[:, :, 2].astype(BF16)
    places = jnp.arange(full_len, dtype=jnp.int32)
    segment = jnp.sum((doc_starts[:, None, :] <= places[None, :, None]).astype(jnp.int32), axis=2)
    heads_out, sums_log = lax.map(
        lambda item: forward_stream(*item, scale), (query, keys, values, segment)
    )
    merged = heads_out.reshape(count, head_width)
    up = dot(second, up_w, ((1,), (0,))) + bias_u
    active_f32, gelu_pullback = jax.vjp(lambda v: jax.nn.gelu(v, approximate=False), up)
    active = active_f32.astype(BF16)
    partial_out = dot(merged, out_w, ((1,), (0,))) + dot(active, down_w, ((1,), (0,)))
    summed_out = scatter_direct(partial_out.reshape(seq_size, local_len, width), "seq")
    layer_out = (tokens.astype(F32) + summed_out[None] + (bias_o + bias_d)).astype(BF16)

    active_grad = dot(grad, down_w, ((1,), (1,)))
    up_grad = gelu_pullback(active_grad)[0].astype(BF16)
    second_grad = dot(up_grad, up_w, ((1,), (1,)))
    down_grad = dot(active, grad, ((0,), (0,)))
    up_weight_grad = dot(second, up_grad, ((0,), (0,)))
    output_weight_grad = dot(merged, grad, ((0,), (0,)))
    heads_grad = dot(grad, out_w, ((1,), (1,))).astype(BF16)
    heads_grad = heads_grad.reshape(streams, full_len, local_heads, HEAD_DIM)
    query_grad, key_grad, value_grad = lax.map(
        lambda item: backward_stream(*item, scale),
        (query, keys, values, segment, sums_log, heads_grad),
    )
    query_back = rotate(query_grad.astype(F32), cosine, sine, -1.0).astype(BF16)
    keys_back = rotate(key_grad.astype(F32), cosine, sine, -1.0).astype(BF16)
    mixed_grad = jnp.stack([query_back, keys_back, value_grad], axis=2).reshape(count, 3 * head_width)
    joint_weight_grad = dot(first, mixed_grad, ((0,), (0,)))
    first_grad = dot(mixed_grad, joint, ((1,), (1,)))

    incoming = first_grad * gain_a + second_grad * gain_f
    incoming = scatter_direct(incoming.reshape(seq_size, local_len, width), "seq")[None]
    own_unit, own_scale = normalised(tokens.astype(F32))
    own_term = own_scale * (
        incoming
        - jnp.mean(incoming, axis=-1, keepdims=True)
        - own_unit * jnp.mean(incoming * own_unit, axis=-1, keepdims=True)
    )
    input_grad = cotangent.astype(F32) + own_term

    first_back, second_back = first_route[::-1], second_route[::-1]

    def scatter_rows(value, order):
        return scatter_bits(value.reshape(batch_size, -1, value.shape[1]), "batch", order, BF16).astype(BF16)

    def column_scatter(value, order):
        return exchange(scatter_rows(value, order).reshape(seq_size, rows, -1), "seq").astype(F32)

    joint_out = (
        column_scatter(joint_weight_grad, first_back)
        .reshape(seq_size, rows, 3, head_width)
        .transpose(1, 2, 0, 3)
        .reshape(rows, -1)
    )
    up_out = (
        column_scatter(up_weight_grad, second_back)
        .reshape(seq_size, rows, batch_size, hidden_rows)
        .transpose(1, 2, 0, 3)
        .reshape(rows, -1)
    )
    down_out = scatter_bits(down_grad.reshape(batch_size, -1, width), "batch", second_back, BF16)
    output_out = lax.ppermute(scatter_rows(output_weight_grad, first_back), both, back).astype(F32)

    own = (jnp.arange(seq_size) == seq_index).astype(F32)
    joint_bias_sum = jnp.sum(mixed_grad.astype(F32), axis=0).reshape(3, 1, head_width) * own[None, :, None]
    up_bias_sum = jnp.sum(up_grad.astype(F32), axis=0).reshape(batch_size, 1, hidden_rows) * own[None, :, None]
    sums = (
        jnp.sum(first_grad * unit, axis=0),
        jnp.sum(first_grad, axis=0),
        jnp.sum(cotangent.astype(F32), axis=(0, 1)),
        jnp.sum(second_grad * unit, axis=0),
        jnp.sum(second_grad, axis=0),
        joint_bias_sum.reshape(-1),
        up_bias_sum.reshape(-1),
    )
    grouped = jnp.concatenate([s.reshape(devices, -1) for s in sums], axis=1)
    mine = scatter_bits(grouped.reshape(batch_size, seq_size, -1), "batch", first_back, F32)
    mine = scatter_bits(mine, "seq", seq_bits, F32)
    small, at = [], 0
    for value in sums:
        size = value.shape[0] // devices
        small.append(mine[at : at + size])
        at += size
    return (
        layer_out,
        input_grad,
        small[0],
        small[1],
        joint_out,
        small[5],
        output_out,
        small[2],
        small[3],
        small[4],
        up_out,
        small[6],
        down_out,
        small[2],
    )


def solution(mesh):
    split = P(("batch", "seq"))
    matrix = P(("batch", "seq"), None)
    rows = P("batch", "seq", None)
    return jax.shard_map(
        body,
        mesh=mesh,
        in_specs=(
            rows, P("batch", None), split, split, matrix, split, matrix, split, split, split, matrix, split,
            matrix, split, rows,
        ),
        out_specs=(
            rows, rows, split, split, matrix, split, matrix, split, split, split, matrix, split, matrix, split,
        ),
        check_vma=False,
    )
```
